32 devices in a mesh: dp: 2 (over x), ctx: 4 (over y, core), tp: 4 (over z).
Axes of the slice: x: 2, y: 2, z: 4, core: 2. Of those that a mesh axis runs over, the one named last changes fastest.
Arguments:
- layer_input: bfloat16 [2, 1024, 8192], P('dp', ('ctx', 'tp')), may hold values from -6 to 6
- value_weight: bfloat16 [8192, 1024], P(('dp', 'ctx'), 'tp'), may hold values from -0.0625 to 0.0625
- query_raw: bfloat16 [2, 1024, 1024], P('dp', 'ctx', 'tp'), may hold values from -6 to 6
- key_raw: bfloat16 [2, 1024, 1024], P('dp', 'ctx', 'tp'), may hold values from -6 to 6
- out_grad: bfloat16 [2, 1024, 1024], P('dp', 'ctx', 'tp'), may hold values from -6 to 6
- gate_logits: float32 [2, 2, 8, 1024], P(None, 'dp', 'tp', 'ctx'), may hold values from -14 to 4, as said below
- decay_params: float32 [2, 8], P(None, 'tp'), may hold values from -0.35 to 0.35
- saved_states: float32 [2, 4, 8, 128, 128], P('dp', 'ctx', 'tp'), may hold values from -4 to 4
Outputs:
- input_grad: bfloat16 [2, 1024, 8192], P('dp', ('ctx', 'tp'))
- query_grad: bfloat16 [2, 1024, 1024], P('dp', 'ctx', 'tp')
- key_grad: bfloat16 [2, 1024, 1024], P('dp', 'ctx', 'tp')
- gate_grad: float32 [2, 2, 8, 1024], P(None, 'dp', 'tp', 'ctx')
- decay_grad: float32 [2, 8], P(None, 'tp')
The draws below stay inside these ranges and needn't reach their ends.
Inputs may be any that keep to these rules, and one draw needn't show every extreme that they name: `gate_logits`: row 0 holds decay logits, row 1 write-strength logits.
All inputs are finite; a program needn't handle non-finite values.
Results may differ from the reference program's by a relative error of at most 0.015.
Values may be sent and summed in bfloat16 or wider, within the bound.
A program may use at most 64 MiB of HBM per device.

```python
import math
import jax
import jax.numpy as jnp
from jax import lax

D = 8192
HD = 128
HEADS_DEV = 2
SUBLEN = 64
TOK_DEV = 256
LOCAL_HEADS = 8
BATCH_SEQUENCES = 2
BLOCKS = 4
SEQUENCE_TOKENS = 1024


def draw_gate_logits(key, part):
    random_subkeys = jax.random.split(key, 8)
    fast_share = 0.5
    shape_head = (BATCH_SEQUENCES, LOCAL_HEADS, 1)
    is_fast = jax.random.uniform(random_subkeys[0], shape_head) < fast_share
    fast_rate = jnp.exp(jax.random.uniform(random_subkeys[1], shape_head, minval=math.log(0.02), maxval=math.log(0.05)))
    slow_rate = jnp.exp(jax.random.uniform(random_subkeys[2], shape_head, minval=math.log(0.1), maxval=math.log(0.5))) / SEQUENCE_TOKENS
    baseline_rate = jnp.where(is_fast, fast_rate, slow_rate)
    block_scaling = jnp.exp(jax.random.uniform(random_subkeys[3], (BATCH_SEQUENCES, LOCAL_HEADS, SEQUENCE_TOKENS // TOK_DEV, 1), minval=math.log(0.5), maxval=math.log(2.0)))
    block_scaling = jnp.broadcast_to(block_scaling, (BATCH_SEQUENCES, LOCAL_HEADS, SEQUENCE_TOKENS // TOK_DEV, TOK_DEV)).reshape(BATCH_SEQUENCES, LOCAL_HEADS, SEQUENCE_TOKENS)
    jaggedness = jnp.exp(jax.random.uniform(random_subkeys[4], (BATCH_SEQUENCES, LOCAL_HEADS, SEQUENCE_TOKENS), minval=math.log(0.5), maxval=math.log(2.0)))
    spike_events = jax.random.uniform(random_subkeys[5], (BATCH_SEQUENCES, LOCAL_HEADS, SEQUENCE_TOKENS)) < 3.0 / SEQUENCE_TOKENS
    spike_rate = jax.random.uniform(random_subkeys[6], (BATCH_SEQUENCES, LOCAL_HEADS, SEQUENCE_TOKENS), minval=0.25, maxval=0.7)
    per_token_rate = baseline_rate * block_scaling * jaggedness + jnp.where(spike_events, spike_rate, 0.0)
    decay_logit = jnp.clip(jnp.log(jnp.expm1(per_token_rate)), -14.0, 1.0)
    strength_logit = jnp.clip(1.5 * jax.random.normal(random_subkeys[7], (BATCH_SEQUENCES, LOCAL_HEADS, SEQUENCE_TOKENS)), -4.0, 4.0)
    return jnp.stack([decay_logit, strength_logit]).astype(jnp.float32)


def block_scale(rng, extent, cuts, least, largest):
    def one(axis_at, shards_of):
        draws = jax.random.uniform(jax.random.fold_in(jax.random.fold_in(rng, 6), axis_at), (shards_of,), jnp.float32, least / len(cuts), largest / len(cuts))
        return jnp.repeat(jnp.exp(draws), extent[axis_at] // shards_of).reshape((-1,) + (1,) * (len(extent) - axis_at - 1))

    loudness = one(*cuts[0])
    for cut in cuts[1:]:
        loudness = loudness * one(*cut)
    return loudness


def centred(own_key, extent, deviation, bound, cuts=(), kind=jnp.bfloat16):
    result = deviation * jax.random.normal(own_key, extent, jnp.float32)
    if cuts:
        result = result * block_scale(own_key, extent, cuts, -0.22, 0.18)
    return jnp.clip(result, -bound, bound).astype(kind)


def setup_inputs(seed: int = 0) -> dict:
    key_of = jax.random.split(jax.random.key(seed), 9)
    layer_input = centred(key_of[0], (BATCH_SEQUENCES, SEQUENCE_TOKENS, D), 1.0, 6.0, ((0, 2), (1, 16)))
    value_weight = centred(key_of[1], (D, LOCAL_HEADS * HD), D ** -0.5, 0.0625, ((0, 8), (1, 4)))
    query_raw = centred(key_of[2], (BATCH_SEQUENCES, SEQUENCE_TOKENS, LOCAL_HEADS * HD), 1.0, 6.0, ((0, 2), (1, 4), (2, 4)))
    key_raw = centred(key_of[3], (BATCH_SEQUENCES, SEQUENCE_TOKENS, LOCAL_HEADS * HD), 1.0, 6.0, ((0, 2), (1, 4), (2, 4)))
    out_grad = centred(key_of[4], (BATCH_SEQUENCES, SEQUENCE_TOKENS, LOCAL_HEADS * HD), 1.0, 6.0, ((0, 2), (1, 4), (2, 4)))
    gate_logits = draw_gate_logits(jax.random.fold_in(key_of[8], 71), 0)
    decay_params = jnp.clip(jax.random.uniform(key_of[6], (2, LOCAL_HEADS), jnp.float32, -0.35, 0.35) * block_scale(key_of[6], (2, LOCAL_HEADS), ((1, 4),), -0.4, 0.0), -0.35, 0.35)
    saved_states = centred(key_of[7], (BATCH_SEQUENCES, BLOCKS, LOCAL_HEADS, HD, HD), 0.5, 4.0, ((0, 2), (1, 4), (2, 4)), jnp.float32)
    return dict(layer_input=layer_input, value_weight=value_weight, query_raw=query_raw, key_raw=key_raw, out_grad=out_grad, gate_logits=gate_logits, decay_params=decay_params, saved_states=saved_states)


epsilon = 1e-06
highest = lax.Precision.HIGHEST

def inner_step(carried, pieces):
    query_unit, key_unit, values, log_decay, strengths = pieces
    sub_len = query_unit.shape[0]
    head_dim = query_unit.shape[1]
    cumulative = jnp.cumsum(log_decay)
    positions = jnp.arange(sub_len)
    lower_mask = positions[:, None] >= positions[None, :]
    strict_mask = positions[:, None] > positions[None, :]
    spread = jnp.where(lower_mask, cumulative[:, None] - cumulative[None, :], 0.0)
    decays = jnp.where(lower_mask, jnp.exp(spread), 0.0)
    key_gram = jnp.dot(key_unit, key_unit.T, precision=highest)
    system = jnp.eye(sub_len, dtype=jnp.float32) + jnp.where(strict_mask, strengths[:, None] * decays * key_gram, 0.0)
    right_side = jnp.concatenate([(strengths * jnp.exp(cumulative))[:, None] * key_unit, strengths[:, None] * values], axis=1)
    solved = jax.scipy.linalg.solve_triangular(system, right_side, lower=True, unit_diagonal=True)
    new_values = solved[:, head_dim:] - jnp.dot(solved[:, :head_dim], carried, precision=highest)
    scores = decays * jnp.dot(query_unit, key_unit.T, precision=highest)
    output = jnp.dot(query_unit * jnp.exp(cumulative)[:, None], carried, precision=highest) + jnp.dot(scores, new_values, precision=highest)
    tail_decay = jnp.exp(cumulative[-1] - cumulative)
    updated = jnp.exp(cumulative[-1]) * carried + jnp.dot((key_unit * tail_decay[:, None]).T, new_values, precision=highest)
    return (updated, output)

def core(query_row, key_row, values, gate_a, gate_b, params, initial):
    length = query_row.shape[0]
    head_dim = query_row.shape[1]
    query_unit = query_row * lax.rsqrt(lax.optimization_barrier(jnp.sum(query_row * query_row, axis=-1, keepdims=True)) + epsilon) * head_dim ** (-0.5)
    key_unit = key_row * lax.rsqrt(lax.optimization_barrier(jnp.sum(key_row * key_row, axis=-1, keepdims=True)) + epsilon)
    log_decay = -jnp.exp(params[0]) * jax.nn.softplus(gate_a + params[1])
    strengths = jax.nn.sigmoid(gate_b)
    blocks = length // SUBLEN

    def into_blocks(array):
        return array.reshape((blocks, SUBLEN) + array.shape[1:])
    final_state, outputs = lax.scan(inner_step, initial, (into_blocks(query_unit), into_blocks(key_unit), into_blocks(values), into_blocks(log_decay), into_blocks(strengths)))
    return (outputs.reshape(length, head_dim), final_state)

def reference(layer_input, value_weight, query_raw, key_raw, out_grad, gate_logits, decay_params, saved_states):
    batch_core = jax.vmap(core, in_axes=(0, 0, 0, 0, 0, None, 0))

    def one_head(head_index):
        columns = lax.dynamic_slice_in_dim(value_weight, head_index * HD, HD, 1)
        value_round = jnp.dot(layer_input.astype(jnp.float32), columns.astype(jnp.float32), preferred_element_type=jnp.float32).astype(jnp.bfloat16)
        value_head = value_round.astype(jnp.float32)
        query_head = lax.dynamic_slice_in_dim(query_raw, head_index * HD, HD, 2).astype(jnp.float32)
        key_head = lax.dynamic_slice_in_dim(key_raw, head_index * HD, HD, 2).astype(jnp.float32)
        grad_head = lax.dynamic_slice_in_dim(out_grad, head_index * HD, HD, 2).astype(jnp.float32)
        gates = lax.dynamic_index_in_dim(gate_logits, head_index, 2, keepdims=False)
        params = lax.dynamic_index_in_dim(decay_params, head_index, 1, keepdims=False)
        states = lax.dynamic_index_in_dim(saved_states, head_index, 2, keepdims=False)
        incoming = jnp.zeros((BATCH_SEQUENCES, HD, HD), jnp.float32)
        param_grad = jnp.zeros((2,), jnp.float32)
        collected = []
        for block_index in reversed(range(BLOCKS)):
            begin = block_index * TOK_DEV
            finish = begin + TOK_DEV
            outputs, pullback = jax.vjp(batch_core, query_head[:, begin:finish], key_head[:, begin:finish], value_head[:, begin:finish], gates[0][:, begin:finish], gates[1][:, begin:finish], params, states[:, block_index])
            gradients = pullback((grad_head[:, begin:finish], incoming))
            incoming = gradients[6]
            param_grad = param_grad + gradients[5]
            collected.append(gradients)
        collected = collected[::-1]
        query_part = jnp.concatenate([part_grads[0] for part_grads in collected], axis=1).astype(jnp.bfloat16)
        key_part = jnp.concatenate([part_grads[1] for part_grads in collected], axis=1).astype(jnp.bfloat16)
        value_part = jnp.concatenate([part_grads[2] for part_grads in collected], axis=1).astype(jnp.bfloat16)
        decay_part = jnp.concatenate([part_grads[3] for part_grads in collected], axis=1)
        strength_part = jnp.concatenate([part_grads[4] for part_grads in collected], axis=1)
        gate_part = jnp.stack([decay_part, strength_part])
        contribution = jnp.einsum('bsc,dc->bsd', value_part.astype(jnp.float32), columns.astype(jnp.float32), precision=highest)
        return (contribution, (query_part, key_part, gate_part, param_grad))

    def one_group(summed_grad, group_index):
        group_sum = jnp.zeros((BATCH_SEQUENCES, SEQUENCE_TOKENS, D), jnp.float32)
        parts = []
        for offset in range(HEADS_DEV):
            contribution, head_parts = one_head(group_index * HEADS_DEV + offset)
            group_sum = group_sum + contribution
            parts.append(head_parts)
        rounded = lax.optimization_barrier(group_sum.astype(jnp.bfloat16))
        summed_grad = summed_grad + rounded.astype(jnp.float32)
        stacked = tuple((jnp.stack([head_parts[index] for head_parts in parts]) for index in range(4)))
        return (summed_grad, stacked)
    summed, per_group = lax.scan(one_group, jnp.zeros((BATCH_SEQUENCES, SEQUENCE_TOKENS, D), jnp.float32), jnp.arange(LOCAL_HEADS // HEADS_DEV, dtype=jnp.int32))
    per_head = tuple((array.reshape((LOCAL_HEADS,) + array.shape[2:]) for array in per_group))
    query_grad = per_head[0].transpose(1, 2, 0, 3).reshape(BATCH_SEQUENCES, SEQUENCE_TOKENS, LOCAL_HEADS * HD)
    key_grad = per_head[1].transpose(1, 2, 0, 3).reshape(BATCH_SEQUENCES, SEQUENCE_TOKENS, LOCAL_HEADS * HD)
    gate_grad = per_head[2].transpose(1, 2, 0, 3)
    decay_grad = per_head[3].T
    return (summed.astype(jnp.bfloat16), query_grad, key_grad, gate_grad, decay_grad)
```

```python
import functools

import jax
import jax.numpy as jnp
from jax import lax
from jax.experimental import pallas as pl
from jax.experimental.pallas import tpu as pltpu
from jax.sharding import PartitionSpec as P

epsilon = 1e-06
f32, bf16 = jnp.float32, jnp.bfloat16
NN, NT, TN = ((1,), (0,)), ((1,), (1,)), ((0,), (0,))
ROWS = ("dp", "ctx")


def mm(a, b, dims=NN):
    return lax.dot_general(
        a.astype(bf16), b.astype(bf16), (dims, ((), ())), preferred_element_type=f32
    )


def halves(a):
    high = a.astype(bf16)
    return high, (a - high.astype(f32)).astype(bf16)


def mm3(a, b):
    (ah, al), (bh, bl) = a, b
    return mm(ah, bh) + (mm(ah, bl) + mm(al, bh))


def grid_of(n):
    rows = lax.broadcasted_iota(jnp.int32, (n, n), 0)
    cols = lax.broadcasted_iota(jnp.int32, (n, n), 1)
    return rows, cols


def to_col(row, eye):
    return jnp.sum(jnp.where(eye, row, 0.0), axis=1, keepdims=True)


def to_row(col, eye):
    return jnp.sum(jnp.where(eye, col, 0.0), axis=0, keepdims=True)


def decay_of(log_row, rows, cols):
    cum = jnp.sum(jnp.where(cols <= rows, log_row, 0.0), axis=1, keepdims=True)
    cum_row = to_row(cum, rows == cols)
    lower = rows >= cols
    decays = jnp.where(lower, jnp.exp(jnp.where(lower, cum - cum_row, 0.0)), 0.0)
    last = cum[-1:, :]
    return decays, jnp.exp(cum), jnp.exp(last - cum), jnp.exp(last)


def unit(raw):
    raw = raw.astype(f32)
    inv = lax.rsqrt(jnp.sum(raw * raw, axis=1, keepdims=True) + epsilon)
    return raw * inv, inv


def inverse(system, rows, cols):
    size, n = 1, system.shape[0]
    result = jnp.where(rows == cols, 1.0, 0.0)
    while size < n:
        pair = jnp.logical_and(rows // (2 * size) == cols // (2 * size), rows // size > cols // size)
        part = jnp.where(pair, system, 0.0)
        if size == 1:
            result = result - part
        else:
            split = halves(result)
            result = result - mm3(split, halves(mm3(halves(part), split)))
        size *= 2
    return result


def maps_kernel(heads, q_ref, k_ref, do_ref, gate_ref, maps_ref, solve_ref):
    n, width = q_ref.shape
    d = width // heads
    rows, cols = grid_of(n)
    srows, scols = grid_of(d)
    for h in range(heads):
        at = slice(h * d, (h + 1) * d)
        query = unit(q_ref[:, at])[0] * d**-0.5
        key = unit(k_ref[:, at])[0]
        do = do_ref[:, at]
        decays, grow, tail, total = decay_of(gate_ref[h : h + 1, :], rows, cols)
        strength = to_col(gate_ref[heads + h : heads + h + 1, :], rows == cols)
        system = jnp.where(rows > cols, strength * decays * mm(key, key, NT), 0.0)
        solve = inverse(system, rows, cols)
        solve_ref[h] = solve.astype(bf16)
        scores = decays * mm(query, key, NT)
        weights = mm(solve, strength * grow * key)
        matrix = jnp.where(srows == scols, total, 0.0) - mm(weights, tail * key, TN)
        local = mm(grow * query, do, TN) - mm(weights, mm(scores, do, TN), TN)
        maps_ref[h, 0] = matrix.astype(bf16)
        maps_ref[h, 1] = local.astype(bf16)


def value_kernel(
    heads, place_ref, q_ref, k_ref, do_ref, gate_ref, solve_ref, all_ref, dv_ref, dr_ref, inc_ref
):
    n, width = q_ref.shape
    d = width // heads
    place = place_ref[0]
    rows, cols = grid_of(n)
    for h in range(heads):
        at = slice(h * d, (h + 1) * d)
        incoming = jnp.zeros((d, d), f32)
        for later in reversed(range(1, all_ref.shape[0])):
            high, low = halves(incoming)
            matrix = all_ref[later, h, 0]
            new = mm(matrix, high) + mm(matrix, low) + all_ref[later, h, 1].astype(f32)
            incoming = jnp.where(later > place, new, incoming)
        inc_ref[h] = incoming
        query = unit(q_ref[:, at])[0] * d**-0.5
        key = unit(k_ref[:, at])[0]
        decays, grow, tail, total = decay_of(gate_ref[h : h + 1, :], rows, cols)
        strength = to_col(gate_ref[heads + h : heads + h + 1, :], rows == cols)
        scores = decays * mm(query, key, NT)
        dn = mm(scores, do_ref[:, at], TN) + mm(tail * key, incoming)
        dr = mm(solve_ref[h], dn, TN)
        dr_ref[:, at] = dr
        dv_ref[:, at] = (strength * dr).astype(bf16)


def grads_kernel(
    heads, q_ref, k_ref, do_ref, gate_ref, solve_ref, dr_ref, inc_ref, state_ref, v_ref,
    dq_ref, dk_ref, dgate_ref,
):
    n, width = q_ref.shape
    d = width // heads
    rows, cols = grid_of(n)
    eye = rows == cols
    lower = rows >= cols
    strict = rows > cols
    scale = d**-0.5

    def gate(kind, h):
        return gate_ref[kind * heads + h : kind * heads + h + 1, :]

    def rowsum(a):
        return jnp.sum(a, axis=1, keepdims=True)

    for h in range(heads):
        at = slice(h * d, (h + 1) * d)
        qh, qinv = unit(q_ref[:, at])
        key, kinv = unit(k_ref[:, at])
        query = qh * scale
        do = do_ref[:, at]
        decays, grow, tail, total = decay_of(gate(0, h), rows, cols)
        strength = to_col(gate(1, h), eye)
        state = state_ref[h]
        incoming = inc_ref[h]
        dr = dr_ref[:, at]
        held = mm(key, state)
        gap = v_ref[:, at].astype(f32) - grow * held
        new = mm(solve_ref[h], strength * gap)
        from_state = mm(do, state, NT)
        dscores = jnp.where(lower, mm(do, new, NT), 0.0)
        dsystem = jnp.where(strict, -mm(dr, new, NT), 0.0)
        gram = mm(key, key, NT)
        scores = decays * mm(query, key, NT)
        ds = dscores * decays
        dsd = dsystem * decays
        dgram = dsd * strength
        dq = grow * from_state + mm(ds, key)
        new_inc = mm(new, incoming, NT)
        dk = (
            tail * new_inc
            + mm(ds, query, TN)
            - strength * grow * mm(dr, state, NT)
            + mm(dgram, key)
            + mm(dgram, key, TN)
        )
        mix = dsd * gram
        dstrength = rowsum(dr * gap) + rowsum(mix)
        spread = dscores * scores + mix * strength
        tails = tail * rowsum(key * new_inc)
        dcum = (
            grow * (rowsum(query * from_state) - strength * rowsum(dr * held))
            + rowsum(spread)
            - tails
            - to_col(jnp.sum(spread, axis=0, keepdims=True), eye)
        )
        end = jnp.sum(tails, axis=0, keepdims=True) + total * jnp.sum(
            rowsum(incoming * state), axis=0, keepdims=True
        )
        dlog = jnp.sum(jnp.where(lower, dcum, 0.0), axis=0, keepdims=True) + end
        dq_ref[:, at] = (qinv * scale * (dq - qh * rowsum(qh * dq))).astype(bf16)
        dk_ref[:, at] = (kinv * (dk - key * rowsum(key * dk))).astype(bf16)
        dgate_ref[h : h + 1, :] = dlog * gate(2, h)
        dgate_ref[heads + h : heads + h + 1, :] = to_row(dstrength, eye) * gate(3, h)
        dgate_ref[2 * heads + h : 2 * heads + h + 1, :] = dlog * gate(0, h)


def call(kernel, outs, in_count, flops, smem=0):
    return pl.pallas_call(
        kernel,
        out_shape=outs,
        in_specs=[pl.BlockSpec(memory_space=pltpu.SMEM)] * smem
        + [pl.BlockSpec(memory_space=pltpu.VMEM)] * in_count,
        out_specs=[pl.BlockSpec(memory_space=pltpu.VMEM)] * len(outs),
        compiler_params=pltpu.CompilerParams(vmem_limit_bytes=32 * 1024 * 1024),
        cost_estimate=pl.CostEstimate(flops=flops, bytes_accessed=2**21, transcendentals=2**17),
    )


def per_device(
    layer_input, value_weight, query_raw, key_raw, out_grad, gate_logits, decay_params, saved_states
):
    tp = lax.axis_size("tp")
    shape = jax.ShapeDtypeStruct
    query, key, do = query_raw[0], key_raw[0], out_grad[0]
    n, width = query.shape
    d = saved_states.shape[-1]
    heads = width // d
    tokens = layer_input.shape[1]

    weights = lax.all_gather(value_weight, "tp")
    sliced = lax.all_to_all(layer_input[0], ROWS, split_axis=1, concat_axis=0, tiled=True)

    scale = -jnp.exp(decay_params[0])[:, None]
    logit = gate_logits[0, 0] + decay_params[1][:, None]
    strength = jax.nn.sigmoid(gate_logits[1, 0])
    gates = jnp.concatenate(
        [
            scale * jax.nn.softplus(logit),
            strength,
            scale * jax.nn.sigmoid(logit),
            strength * (1.0 - strength),
        ]
    )
    maps, solve = call(
        functools.partial(maps_kernel, heads),
        [shape((heads, 2, d, d), bf16), shape((heads, n, n), bf16)],
        4,
        2**33,
    )(query, key, do, gates)
    everything = lax.all_gather(maps, "ctx")
    place = lax.axis_index("ctx").astype(jnp.int32)[None]
    dv, dr, incoming = call(
        functools.partial(value_kernel, heads),
        [shape((n, width), bf16), shape((n, width), f32), shape((heads, d, d), f32)],
        6,
        2**31,
        1,
    )(place, query, key, do, gates, solve, everything)

    partial = lax.dot_general(
        sliced, weights, (((1,), (1,)), ((), ())), preferred_element_type=f32
    ).astype(bf16)
    summed = lax.psum_scatter(partial, ROWS, scatter_dimension=0, tiled=True)
    values = lax.all_to_all(summed, "tp", split_axis=1, concat_axis=0, tiled=True)
    values = values.reshape(n, width)

    turned = lax.all_to_all(dv.reshape(tp, tokens, width), "tp", split_axis=0, concat_axis=0)
    wide = lax.all_gather(turned.reshape(tp, tokens, width), ROWS)
    product = jnp.einsum("ntlc,tdc->nld", wide, weights, preferred_element_type=f32).astype(bf16)
    input_grad = lax.all_to_all(product, ROWS, split_axis=0, concat_axis=2, tiled=True)
    input_grad = input_grad.reshape(1, tokens, layer_input.shape[2])

    dq, dk, dgate = call(
        functools.partial(grads_kernel, heads),
        [shape((n, width), bf16), shape((n, width), bf16), shape((3 * heads, n), f32)],
        9,
        2**32,
    )(query, key, do, gates, solve, dr, incoming, saved_states[0, 0], values)
    gate_grad = dgate[: 2 * heads].reshape(2, 1, heads, n)
    sums = jnp.sum(dgate.reshape(3, heads, n), axis=2)
    decay_grad = lax.psum(jnp.stack([sums[2], sums[0]]), ROWS)
    return (input_grad, dq[None], dk[None], gate_grad, decay_grad)


def solution(mesh):
    placed = (
        P("dp", ("ctx", "tp"), None),
        P(("dp", "ctx"), "tp"),
        P("dp", "ctx", "tp"),
        P("dp", "ctx", "tp"),
        P("dp", "ctx", "tp"),
        P(None, "dp", "tp", "ctx"),
        P(None, "tp"),
        P("dp", "ctx", "tp", None, None),
    )
    return jax.shard_map(
        per_device,
        mesh=mesh,
        in_specs=placed,
        out_specs=(
            P("dp", ("ctx", "tp"), None),
            P("dp", "ctx", "tp"),
            P("dp", "ctx", "tp"),
            P(None, "dp", "tp", "ctx"),
            P(None, "tp"),
        ),
        check_vma=False,
    )
```

```python
import functools

import jax
import jax.numpy as jnp
from jax import lax
from jax.experimental import pallas as pl
from jax.experimental.pallas import tpu as pltpu
from jax.sharding import PartitionSpec as P

epsilon = 1e-06
f32, bf16 = jnp.float32, jnp.bfloat16
NN, NT, TN = ((1,), (0,)), ((1,), (1,)), ((0,), (0,))
ROWS = ("dp", "ctx")


def mm(a, b, dims=NN):
    return lax.dot_general(
        a.astype(bf16), b.astype(bf16), (dims, ((), ())), preferred_element_type=f32
    )


def halves(a):
    high = a.astype(bf16)
    return high, (a - high.astype(f32)).astype(bf16)


def mm3(a, b):
    (ah, al), (bh, bl) = a, b
    return mm(ah, bh) + (mm(ah, bl) + mm(al, bh))


def grid_of(n):
    rows = lax.broadcasted_iota(jnp.int32, (n, n), 0)
    cols = lax.broadcasted_iota(jnp.int32, (n, n), 1)
    return rows, cols


def to_col(row, eye):
    return jnp.sum(jnp.where(eye, row, 0.0), axis=1, keepdims=True)


def to_row(col, eye):
    return jnp.sum(jnp.where(eye, col, 0.0), axis=0, keepdims=True)


def decay_of(log_row, rows, cols):
    cum = jnp.sum(jnp.where(cols <= rows, log_row, 0.0), axis=1, keepdims=True)
    cum_row = to_row(cum, rows == cols)
    lower = rows >= cols
    decays = jnp.where(lower, jnp.exp(jnp.where(lower, cum - cum_row, 0.0)), 0.0)
    last = cum[-1:, :]
    return decays, jnp.exp(cum), jnp.exp(last - cum), jnp.exp(last)


def unit(raw):
    raw = raw.astype(f32)
    inv = lax.rsqrt(jnp.sum(raw * raw, axis=1, keepdims=True) + epsilon)
    return raw * inv, inv


def inverse(system, rows, cols):
    size, n = 1, system.shape[0]
    result = jnp.where(rows == cols, 1.0, 0.0)
    while size < n:
        pair = jnp.logical_and(rows // (2 * size) == cols // (2 * size), rows // size > cols // size)
        part = jnp.where(pair, system, 0.0)
        if size == 1:
            result = result - part
        else:
            split = halves(result)
            result = result - mm3(split, halves(mm3(halves(part), split)))
        size *= 2
    return result


def maps_kernel(heads, q_ref, k_ref, do_ref, gate_ref, maps_ref, solve_ref):
    n, width = q_ref.shape
    d = width // heads
    rows, cols = grid_of(n)
    srows, scols = grid_of(d)
    for h in range(heads):
        at = slice(h * d, (h + 1) * d)
        query = unit(q_ref[:, at])[0] * d**-0.5
        key = unit(k_ref[:, at])[0]
        do = do_ref[:, at]
        decays, grow, tail, total = decay_of(gate_ref[h : h + 1, :], rows, cols)
        strength = to_col(gate_ref[heads + h : heads + h + 1, :], rows == cols)
        system = jnp.where(rows > cols, strength * decays * mm(key, key, NT), 0.0)
        solve = inverse(system, rows, cols)
        solve_ref[h] = solve.astype(bf16)
        scores = decays * mm(query, key, NT)
        weights = mm(solve, strength * grow * key)
        matrix = jnp.where(srows == scols, total, 0.0) - mm(weights, tail * key, TN)
        local = mm(grow * query, do, TN) - mm(weights, mm(scores, do, TN), TN)
        maps_ref[h, 0] = matrix.astype(bf16)
        maps_ref[h, 1] = local.astype(bf16)


def value_kernel(
    heads, place_ref, q_ref, k_ref, do_ref, gate_ref, solve_ref, all_ref, dv_ref, dr_ref, inc_ref
):
    n, width = q_ref.shape
    d = width // heads
    place = place_ref[0]
    rows, cols = grid_of(n)
    for h in range(heads):
        at = slice(h * d, (h + 1) * d)
        incoming = jnp.zeros((d, d), f32)
        for later in reversed(range(1, all_ref.shape[0])):
            high, low = halves(incoming)
            matrix = all_ref[later, h, 0]
            new = mm(matrix, high) + mm(matrix, low) + all_ref[later, h, 1].astype(f32)
            incoming = jnp.where(later > place, new, incoming)
        inc_ref[h] = incoming
        query = unit(q_ref[:, at])[0] * d**-0.5
        key = unit(k_ref[:, at])[0]
        decays, grow, tail, total = decay_of(gate_ref[h : h + 1, :], rows, cols)
        strength = to_col(gate_ref[heads + h : heads + h + 1, :], rows == cols)
        scores = decays * mm(query, key, NT)
        dn = mm(scores, do_ref[:, at], TN) + mm(tail * key, incoming)
        dr = mm(solve_ref[h], dn, TN)
        dr_ref[:, at] = dr
        dv_ref[:, at] = (strength * dr).astype(bf16)


def grads_kernel(
    heads, q_ref, k_ref, do_ref, gate_ref, solve_ref, dr_ref, inc_ref, state_ref, v_ref,
    dq_ref, dk_ref, dgate_ref,
):
    n, width = q_ref.shape
    d = width // heads
    rows, cols = grid_of(n)
    eye = rows == cols
    lower = rows >= cols
    strict = rows > cols
    scale = d**-0.5

    def gate(kind, h):
        return gate_ref[kind * heads + h : kind * heads + h + 1, :]

    def rowsum(a):
        return jnp.sum(a, axis=1, keepdims=True)

    for h in range(heads):
        at = slice(h * d, (h + 1) * d)
        qh, qinv = unit(q_ref[:, at])
        key, kinv = unit(k_ref[:, at])
        query = qh * scale
        do = do_ref[:, at]
        decays, grow, tail, total = decay_of(gate(0, h), rows, cols)
        strength = to_col(gate(1, h), eye)
        state = state_ref[h]
        incoming = inc_ref[h]
        dr = dr_ref[:, at]
        held = mm(key, state)
        gap = v_ref[:, at].astype(f32) - grow * held
        new = mm(solve_ref[h], strength * gap)
        from_state = mm(do, state, NT)
        dscores = jnp.where(lower, mm(do, new, NT), 0.0)
        dsystem = jnp.where(strict, -mm(dr, new, NT), 0.0)
        gram = mm(key, key, NT)
        scores = decays * mm(query, key, NT)
        ds = dscores * decays
        dsd = dsystem * decays
        dgram = dsd * strength
        dq = grow * from_state + mm(ds, key)
        new_inc = mm(new, incoming, NT)
        dk = (
            tail * new_inc
            + mm(ds, query, TN)
            - strength * grow * mm(dr, state, NT)
            + mm(dgram, key)
            + mm(dgram, key, TN)
        )
        mix = dsd * gram
        dstrength = rowsum(dr * gap) + rowsum(mix)
        spread = dscores * scores + mix * strength
        tails = tail * rowsum(key * new_inc)
        dcum = (
            grow * (rowsum(query * from_state) - strength * rowsum(dr * held))
            + rowsum(spread)
            - tails
            - to_col(jnp.sum(spread, axis=0, keepdims=True), eye)
        )
        end = jnp.sum(tails, axis=0, keepdims=True) + total * jnp.sum(
            rowsum(incoming * state), axis=0, keepdims=True
        )
        dlog = jnp.sum(jnp.where(lower, dcum, 0.0), axis=0, keepdims=True) + end
        dq_ref[:, at] = (qinv * scale * (dq - qh * rowsum(qh * dq))).astype(bf16)
        dk_ref[:, at] = (kinv * (dk - key * rowsum(key * dk))).astype(bf16)
        dgate_ref[h : h + 1, :] = dlog * gate(2, h)
        dgate_ref[heads + h : heads + h + 1, :] = to_row(dstrength, eye) * gate(3, h)
        dgate_ref[2 * heads + h : 2 * heads + h + 1, :] = dlog * gate(0, h)


def call(kernel, outs, in_count, flops, smem=0):
    return pl.pallas_call(
        kernel,
        out_shape=outs,
        in_specs=[pl.BlockSpec(memory_space=pltpu.SMEM)] * smem
        + [pl.BlockSpec(memory_space=pltpu.VMEM)] * in_count,
        out_specs=[pl.BlockSpec(memory_space=pltpu.VMEM)] * len(outs),
        compiler_params=pltpu.CompilerParams(vmem_limit_bytes=32 * 1024 * 1024),
        cost_estimate=pl.CostEstimate(flops=flops, bytes_accessed=2**21, transcendentals=2**17),
    )


def spot_of(axes, flat):
    spot = {}
    for name in reversed(axes):
        size = lax.axis_size(name)
        spot[name] = lax.rem(flat, size)
        flat = flat // size
    return spot


def exchange_kernel(axes, share, count, src_ref, dst_ref, send_sem, recv_sem, own_sem):
    me = jnp.int32(0)
    for name in axes:
        me = me * lax.axis_size(name) + lax.axis_index(name)
    barrier = pltpu.get_barrier_semaphore()

    def greet(step, carry):
        peer = lax.rem(me + step, count)
        pl.semaphore_signal(
            barrier, inc=1, device_id=spot_of(axes, peer), device_id_type=pl.DeviceIdType.MESH
        )
        return carry

    lax.fori_loop(1, count, greet, 0)
    own = pltpu.make_async_copy(src_ref.at[me // share], dst_ref.at[me], own_sem)
    own.start()
    pl.semaphore_wait(barrier, count - 1)

    def copy_of(step):
        peer = lax.rem(me + step, count)
        return pltpu.make_async_remote_copy(
            src_ref=src_ref.at[peer // share],
            dst_ref=dst_ref.at[me],
            send_sem=send_sem.at[step],
            recv_sem=recv_sem.at[step],
            device_id=spot_of(axes, peer),
            device_id_type=pl.DeviceIdType.MESH,
        )

    def begin(step, carry):
        copy_of(step).start()
        return carry

    def finish(step, carry):
        source = lax.rem(me + count - step, count)
        pltpu.make_async_remote_copy(
            src_ref=src_ref.at[lax.rem(me + step, count) // share],
            dst_ref=dst_ref.at[source],
            send_sem=send_sem.at[step],
            recv_sem=recv_sem.at[step],
            device_id=spot_of(axes, lax.rem(me + step, count)),
            device_id_type=pl.DeviceIdType.MESH,
        ).wait()
        return carry

    lax.fori_loop(1, count, begin, 0)
    own.wait()
    lax.fori_loop(1, count, finish, 0)


def exchange(source, axes, number, share=1):
    count = 1
    for name in axes:
        count *= lax.axis_size(name)
    block = source.shape[1:]
    return pl.pallas_call(
        functools.partial(exchange_kernel, axes, share, count),
        out_shape=jax.ShapeDtypeStruct((count, *block), source.dtype),
        in_specs=[pl.BlockSpec(memory_space=pltpu.VMEM)],
        out_specs=pl.BlockSpec(memory_space=pltpu.VMEM),
        scratch_shapes=[
            pltpu.SemaphoreType.DMA((count,)),
            pltpu.SemaphoreType.DMA((count,)),
            pltpu.SemaphoreType.DMA,
        ],
        compiler_params=pltpu.CompilerParams(
            collective_id=number, has_side_effects=True, vmem_limit_bytes=32 * 1024 * 1024
        ),
        cost_estimate=pl.CostEstimate(flops=2**33, bytes_accessed=2**22, transcendentals=0),
    )(source)


def per_device(
    layer_input, value_weight, query_raw, key_raw, out_grad, gate_logits, decay_params, saved_states
):
    tp = lax.axis_size("tp")
    shape = jax.ShapeDtypeStruct
    query, key, do = query_raw[0], key_raw[0], out_grad[0]
    n, width = query.shape
    d = saved_states.shape[-1]
    heads = width // d
    tokens = layer_input.shape[1]

    weights = lax.all_gather(value_weight, "tp")
    sliced = lax.all_to_all(layer_input[0], ROWS, split_axis=1, concat_axis=0, tiled=True)

    scale = -jnp.exp(decay_params[0])[:, None]
    logit = gate_logits[0, 0] + decay_params[1][:, None]
    strength = jax.nn.sigmoid(gate_logits[1, 0])
    gates = jnp.concatenate(
        [
            scale * jax.nn.softplus(logit),
            strength,
            scale * jax.nn.sigmoid(logit),
            strength * (1.0 - strength),
        ]
    )
    maps, solve = call(
        functools.partial(maps_kernel, heads),
        [shape((heads, 2, d, d), bf16), shape((heads, n, n), bf16)],
        4,
        2**33,
    )(query, key, do, gates)
    everything = lax.all_gather(maps, "ctx")
    place = lax.axis_index("ctx").astype(jnp.int32)[None]
    dv, dr, incoming = call(
        functools.partial(value_kernel, heads),
        [shape((n, width), bf16), shape((n, width), f32), shape((heads, d, d), f32)],
        6,
        2**31,
        1,
    )(place, query, key, do, gates, solve, everything)

    rows = lax.axis_size("dp") * lax.axis_size("ctx")
    everyone = ("tp", *ROWS)
    wide = exchange(dv.reshape(tp, tokens, width), everyone, 0, rows)
    wide = wide.reshape(tp, rows, tokens, width)
    product = jnp.einsum("tnlc,tdc->nld", wide, weights, preferred_element_type=f32).astype(bf16)
    partial = jnp.einsum("nd,tdc->tnc", sliced, weights, preferred_element_type=f32).astype(bf16)
    parts = exchange(partial.reshape(tp * rows, tokens, width), everyone, 1)
    values = jnp.sum(parts.reshape(tp, rows, tokens, width).astype(f32), axis=1).astype(bf16)
    values = values.reshape(n, width)
    turned = exchange(product, ROWS, 2)
    input_grad = turned.transpose(1, 0, 2).reshape(1, tokens, layer_input.shape[2])

    dq, dk, dgate = call(
        functools.partial(grads_kernel, heads),
        [shape((n, width), bf16), shape((n, width), bf16), shape((3 * heads, n), f32)],
        9,
        2**32,
    )(query, key, do, gates, solve, dr, incoming, saved_states[0, 0], values)
    gate_grad = dgate[: 2 * heads].reshape(2, 1, heads, n)
    sums = jnp.sum(dgate.reshape(3, heads, n), axis=2)
    local = jnp.stack([sums[2], sums[0]])
    local = jnp.pad(local, ((0, 6), (0, 128 - heads)))[None]
    decay_grad = jnp.sum(exchange(local, ROWS, 3, rows)[:, :2, :heads], axis=0)
    return (input_grad, dq[None], dk[None], gate_grad, decay_grad)


def solution(mesh):
    placed = (
        P("dp", ("ctx", "tp"), None),
        P(("dp", "ctx"), "tp"),
        P("dp", "ctx", "tp"),
        P("dp", "ctx", "tp"),
        P("dp", "ctx", "tp"),
        P(None, "dp", "tp", "ctx"),
        P(None, "tp"),
        P("dp", "ctx", "tp", None, None),
    )
    return jax.shard_map(
        per_device,
        mesh=mesh,
        in_specs=placed,
        out_specs=(
            P("dp", ("ctx", "tp"), None),
            P("dp", "ctx", "tp"),
            P("dp", "ctx", "tp"),
            P(None, "dp", "tp", "ctx"),
            P(None, "tp"),
        ),
        check_vma=False,
    )
```
